128 devices in a mesh: groups: 4 (over x, y), samp: 32 (over z, core).
Axes of the slice: x: 2, y: 2, z: 16, core: 2. Of those that a mesh axis runs over, the one named last changes fastest.
The devices are a block of a 8x8x16 slice.
Arguments:
- dosage: bfloat16 [32768, 8192], P(('groups', 'samp')), parts along dimension 0, may hold values from 0 to 2
- covariates: bfloat16 [32768, 96], P(('groups', 'samp')), parts along dimension 0, may hold values from -8 to 8
- expression: bfloat16 [32768, 16384], P('groups', 'samp'), parts along dimension 0, may hold values from -10 to 10
- block_index: int32 [8, 1024], P('groups'), parts along dimension 0, may hold values from 0 to 8191
- expr_row: int32 [32768], P('groups'), parts along dimension 0, may hold values from 0 to 8191, each once
Outputs:
- zscore: float32 [8192, 16384], P('groups', 'samp'), parts along dimension 0
The draws below stay inside these ranges and needn't reach their ends.
There are 4 independent parts, one for each index of `groups`. The reference program is written for one: setup_inputs(seed, part) draws one part's arguments, and reference() takes and returns one part's arrays. A program takes and returns all parts, laid end to end along the dimension named above; each array names one. Nothing has to cross between parts.
Inputs may be any that keep to these rules, and one draw needn't show every extreme that they name: `expr_row`: every expression row appears once.
All inputs are finite; a program needn't handle non-finite values.
Results may differ from the reference program's by a relative error of at most 0.0029.
Values may be sent and summed in bfloat16 or wider, within the bound.
A program may use at most 192 MiB of HBM per device.

```python
import math
import jax
import jax.numpy as jnp
from jax import lax

K = 96
V = 1024
BLOCKS = 2
VPANEL = 8192
NSAMP = 8192
GENES = 16384


def covariate_base(key):
    first = jax.random.fold_in(key, 11)
    normal_part = jax.random.normal(first, (NSAMP, K), jnp.float32)
    rising = 1.0 + 2.0 * jnp.arange(NSAMP, dtype=jnp.float32) / NSAMP
    return jnp.clip(normal_part * rising[:, None], -8.0, 8.0)


def draw_covariates(key, part):
    return covariate_base(key).astype(jnp.bfloat16)


def draw_dosage(key, part):
    base = covariate_base(key)
    loading = jax.random.normal(jax.random.fold_in(key, 21), (K, VPANEL), jnp.float32)
    noise_key = jax.random.fold_in(key, 22)
    noise = jax.random.uniform(noise_key, (NSAMP, VPANEL), jnp.float32, -0.6, 0.6)
    shared = jnp.dot(base, loading) * (0.3 / K ** 0.5)
    return jnp.clip(1.0 + shared + noise, 0.0, 2.0).astype(jnp.bfloat16)


def draw_expression(key, part):
    base = covariate_base(key)
    loading = jax.random.normal(jax.random.fold_in(key, 31), (K, GENES), jnp.float32)
    noise_key = jax.random.fold_in(key, 32)
    noise = jax.random.normal(noise_key, (NSAMP, GENES), jnp.float32)
    shared = jnp.dot(base, loading) * (0.5 / K ** 0.5)
    return jnp.clip(shared + noise, -10.0, 10.0).astype(jnp.bfloat16)


def plant(entries, own_key, least, high):
    place = [jax.random.randint(jax.random.fold_in(own_key, axis), (), 0, length) for axis, length in enumerate(entries.shape)]
    widest = entries.shape.index(max(entries.shape))
    beside = place[:widest] + [(place[widest] + 1) % entries.shape[widest]] + place[widest + 1:]
    return entries.at[tuple(place)].set(least).at[tuple(beside)].set(high)


def setup_inputs(seed: int = 0, part: int = 0) -> dict:
    key_list = jax.random.split(jax.random.key(seed), 6)
    part_keys = jax.random.split(jax.random.fold_in(key_list[5], part), 6)
    dosage = draw_dosage(jax.random.fold_in(jax.random.fold_in(key_list[5], part), 71), part)
    covariates = draw_covariates(jax.random.fold_in(jax.random.fold_in(key_list[5], part), 71), part)
    expression = draw_expression(jax.random.fold_in(jax.random.fold_in(key_list[5], part), 71), part)
    block_index = plant(jax.random.randint(part_keys[3], (BLOCKS, V), 0, VPANEL), jax.random.fold_in(part_keys[3], 1), 0, VPANEL - 1).astype(jnp.int32)
    expr_row = jax.random.permutation(part_keys[4], NSAMP).astype(jnp.int32)
    return dict(dosage=dosage, covariates=covariates, expression=expression, block_index=block_index, expr_row=expr_row)


epsilon = 1e-06

def reference(dosage, covariates, expression, block_index, expr_row):
    gram = jnp.dot(covariates.T.astype(jnp.float32), covariates.astype(jnp.float32), preferred_element_type=jnp.float32)
    factor = jnp.linalg.cholesky(gram)
    matched = jnp.take(expression, expr_row, axis=0)
    panel_norm = lax.optimization_barrier(jnp.sum(jnp.square(expression.astype(jnp.float32)), axis=0))
    cov_float = covariates.astype(jnp.float32)
    scale = math.sqrt(NSAMP - K - 1)
    results = []
    for block in range(BLOCKS):
        picked = jnp.take(dosage, block_index[block], axis=1)
        loads = jnp.dot(covariates.T.astype(jnp.float32), picked.astype(jnp.float32), preferred_element_type=jnp.float32)
        coeffs = jax.scipy.linalg.cho_solve((factor, True), loads)
        fitted = jnp.dot(cov_float, coeffs, precision=lax.Precision.HIGHEST)
        resid = (picked.astype(jnp.float32) - fitted).astype(jnp.bfloat16)
        resid_norm = lax.optimization_barrier(jnp.sum(jnp.square(resid.astype(jnp.float32)), axis=0))
        products = jnp.dot(resid.T.astype(jnp.float32), matched.astype(jnp.float32), preferred_element_type=jnp.float32)
        results.append(scale * products * lax.rsqrt(resid_norm + epsilon)[:, None] * lax.rsqrt(panel_norm + epsilon)[None, :])
    return jnp.concatenate(results, axis=0)
```

```python
import math

import jax
import jax.numpy as jnp
from jax import lax
from jax.sharding import PartitionSpec as P

HIGHEST = lax.Precision.HIGHEST
epsilon = 1e-06


def dot(a, b, contract, precision=None):
    return lax.dot_general(
        a, b, ((contract[:1], contract[1:]), ((), ())), precision=precision, preferred_element_type=jnp.float32
    )


def local(dosage, covariates, expression, block_index, expr_row):
    blocks, width = block_index.shape
    covars = covariates.shape[1]
    genes = expression.shape[1]
    scale = math.sqrt(expr_row.shape[0] - covars - 1)
    gathered = []
    for block in range(blocks):
        picked = jnp.take(dosage, block_index[block], axis=1)
        if block == 0:
            picked = jnp.concatenate([picked, covariates], axis=1)
        gathered.append(lax.all_gather(picked, "samp", axis=0, tiled=True))
    matched = jnp.take(expression, expr_row, axis=0)
    panel_norm = jnp.sum(jnp.square(expression.astype(jnp.float32)), axis=0)
    whole = gathered[0][:, width:]
    gathered[0] = gathered[0][:, :width]
    gram = dot(whole, whole, (0, 0))
    factor = jnp.linalg.cholesky(gram)
    inverse = jax.scipy.linalg.solve_triangular(factor, jnp.eye(covars, dtype=jnp.float32), lower=True)
    cross = dot(whole, matched, (0, 0))
    side = dot(inverse, cross, (1, 0), HIGHEST)
    results = []
    for block in range(blocks):
        picked = gathered[block]
        loads = dot(whole, picked, (0, 0))
        white = dot(inverse, loads, (1, 0), HIGHEST)
        norm = jnp.sum(jnp.square(picked.astype(jnp.float32)), axis=0) - jnp.sum(jnp.square(white), axis=0)
        norm = jnp.maximum(norm, 0.0)
        products = dot(picked, matched, (0, 0)) - dot(white, side, (0, 0), HIGHEST)
        results.append(
            scale * products * lax.rsqrt(norm + epsilon)[:, None] * lax.rsqrt(panel_norm + epsilon)[None, :]
        )
    return jnp.concatenate(results, axis=0)


def solution(mesh):
    in_specs = (P(("groups", "samp"), None), P(("groups", "samp"), None), P("groups", "samp"), P("groups", None), P("groups"))
    return jax.shard_map(local, mesh=mesh, in_specs=in_specs, out_specs=P("groups", "samp"), check_vma=False)
```

```python
import math

import jax
import jax.numpy as jnp
from jax import lax
from jax.experimental import pallas as pl
from jax.experimental.pallas import tpu as pltpu
from jax.sharding import PartitionSpec as P

MESH = pl.DeviceIdType.MESH
HIGHEST = lax.Precision.HIGHEST
F32 = jnp.float32
BF16 = jnp.bfloat16
epsilon = 1e-06
CHUNKS = 8
PARTS = 4


def dot(a, b, contract, precision=None):
    return lax.dot_general(
        a, b, ((contract[:1], contract[1:]), ((), ())), precision=precision, preferred_element_type=F32
    )


def scan_kernel(
    scale, length,
    d_hbm, e_hbm, xt_ref, pick_ref, perm_ref,
    out_hbm, pn_ref,
    a, xt, e, m, d, acc, lac, sq, pacc, kacc, gram, xtm, h,
    ring_send, ring_recv, sib_send, sib_recv, x_send, x_recv, xs_send, xs_recv, load_sem, out_sem,
):
    half = length // 2
    last = half // 2
    end = half - 1
    me = lax.axis_index("samp")
    z = lax.div(me, 2)
    core = lax.rem(me, 2)
    up = lax.rem(me + 2, length)
    down = lax.rem(me + length - 2, length)
    sib = me + 1 - 2 * core
    chunk = a.shape[1] // CHUNKS
    rows = a.shape[2]
    covars = xt.shape[1]
    panel = d.shape[1] // PARTS
    order = e.shape[0] // PARTS

    def place(n):
        s = lax.div(n + 1, 2)
        sign = 2 * lax.rem(n + 1, 2) - 1
        return lax.rem(z + sign * s + half, half)

    def block(q, b):
        return a.at[b, pl.ds(pl.multiple_of(q * chunk, chunk), chunk), :]

    def ring(q, n, target, index, arrival):
        ref = block(q, 2 * place(n) + core)
        return pltpu.make_async_remote_copy(
            src_ref=ref, dst_ref=ref, send_sem=ring_send.at[q, index], recv_sem=ring_recv.at[q, arrival],
            device_id={"samp": target}, device_id_type=MESH,
        )

    def across(q, n):
        ref = block(q, 2 * place(n) + core)
        return pltpu.make_async_remote_copy(
            src_ref=ref, dst_ref=ref, send_sem=sib_send.at[q, n], recv_sem=sib_recv.at[q, n],
            device_id={"samp": sib}, device_id_type=MESH,
        )

    def x_ring(n, target, index, arrival):
        ref = xt.at[2 * place(n) + core]
        return pltpu.make_async_remote_copy(
            src_ref=ref, dst_ref=ref, send_sem=x_send.at[index], recv_sem=x_recv.at[arrival],
            device_id={"samp": target}, device_id_type=MESH,
        )

    def x_across(n):
        ref = xt.at[2 * place(n) + core]
        return pltpu.make_async_remote_copy(
            src_ref=ref, dst_ref=ref, send_sem=xs_send.at[n], recv_sem=xs_recv.at[n],
            device_id={"samp": sib}, device_id_type=MESH,
        )

    def own(q):
        return (ring(q, 0, up, 0, 1), ring(q, 0, down, half, 2), across(q, 0))

    def comm(q, s, parity, link, cross, finish):
        def arrive(n, target, forward):
            if not finish:
                link(n, target, n, n).wait_recv()

            @pl.when(forward)
            def _():
                copy = link(n, target, n, jnp.minimum(n + 2, end))
                copy.wait_send() if finish else copy.start()

            copy = cross(n)
            copy.wait_send() if finish else copy.start()

        @pl.when(s < last)
        def _():
            arrive(2 * s - 1, up, jnp.logical_or(s < last - 1, parity == 0))
            arrive(2 * s, down, jnp.logical_or(s < last - 1, parity == 1))

        @pl.when(s == last)
        def _():
            if not finish:
                link(end, up, end, end).wait_recv()
            copy = cross(end)
            copy.wait_send() if finish else copy.start()

    def chunk_comm(q, s, finish):
        comm(
            q, s, lax.rem(q, 2),
            lambda n, target, index, arrival: ring(q, n, target, index, arrival),
            lambda n: across(q, n), finish,
        )

    def x_comm(s, finish):
        comm(s * 0, s, s * 0, x_ring, x_across, finish)

    def pick(q):
        chosen = pick_ref[pl.ds(q, 1), :]

        def part(k, carry):
            start = pl.multiple_of(k * panel, panel)
            spots = lax.broadcasted_iota(jnp.int32, (panel, chunk), 0) + start
            hot = jnp.where(spots == chosen, 1.0, 0.0).astype(BF16)
            piece = dot(d[:, pl.ds(start, panel)], hot, (1, 0))

            @pl.when(k == 0)
            def _():
                kacc[...] = piece

            @pl.when(k > 0)
            def _():
                kacc[...] += piece

            return carry

        lax.fori_loop(0, PARTS, part, 0)
        a[me, pl.ds(pl.multiple_of(q * chunk, chunk), chunk), :] = kacc[...].T.astype(BF16)

    def permute(i):
        n = lax.div(i, 2)
        b = 2 * place(n) + lax.rem(i, 2)
        wanted = jnp.broadcast_to(perm_ref[pl.ds(b, 1), :], (128, rows)).T[:, :1]

        def part(k, carry):
            start = pl.multiple_of(k * order, order)
            spots = lax.broadcasted_iota(jnp.int32, (rows, order), 1) + start
            hot = jnp.where(spots == wanted, 1.0, 0.0).astype(BF16)
            piece = dot(hot, e[pl.ds(start, order), :], (1, 0))

            @pl.when(k == 0)
            def _():
                pacc[...] = piece

            @pl.when(k > 0)
            def _():
                pacc[...] += piece

            return carry

        lax.fori_loop(0, PARTS, part, 0)
        m[i] = pacc[...].astype(BF16)
        some = e[pl.ds(pl.multiple_of(i * rows, rows), rows), :].astype(F32)
        pn_ref[...] += jnp.sum(some * some, axis=0, keepdims=True)

    def add(q, slot, n):
        across(q, n).wait_recv()
        at = 2 * place(n)
        start = pl.ds(pl.multiple_of(q * chunk, chunk), chunk)
        one, two = a[at, start, :], a[at + 1, start, :]
        acc[slot] += dot(one, m[2 * n], (1, 0)) + dot(two, m[2 * n + 1], (1, 0))
        lac[slot] += dot(one, xt[at], (1, 1)) + dot(two, xt[at + 1], (1, 1))
        one, two = one.astype(F32), two.astype(F32)
        total = one * one + two * two
        sq[slot] += sum(total[:, c : c + 128] for c in range(0, rows, 128)) if rows > 128 else total

    def clear(slot):
        acc[slot] = jnp.zeros(acc.shape[1:], F32)
        lac[slot] = jnp.zeros(lac.shape[1:], F32)
        sq[slot] = jnp.zeros(sq.shape[1:], F32)

    def emit(q, slot):
        return pltpu.make_async_copy(
            acc.at[slot], out_hbm.at[pl.ds(pl.multiple_of(q * chunk, chunk), chunk), :], out_sem.at[q]
        )

    def finish_chunk(q, slot):
        loads = lac[slot]
        white = dot(loads, gram[...], (1, 0), HIGHEST)
        norm = jnp.sum(sq[slot], axis=1, keepdims=True) + jnp.sum(white * loads, axis=1, keepdims=True)
        norm = jnp.maximum(norm, 0.0)
        fitted = dot(loads, h[...], (1, 0), HIGHEST)
        acc[slot] = (acc[slot] + fitted) * (scale * lax.rsqrt(norm + epsilon))
        emit(q, slot).start()

    def sweep(k, carry):
        whole = gram[...]
        row = gram[pl.ds(k, 1), :]
        here = lax.broadcasted_iota(jnp.int32, whole.shape, 1) == k
        there = lax.broadcasted_iota(jnp.int32, whole.shape, 0) == k
        column = jnp.sum(jnp.where(here, whole, 0.0), axis=1, keepdims=True)
        corner = jnp.sum(jnp.where(here[:1], row, 0.0), axis=1, keepdims=True)
        inverse = 1.0 / corner
        scaled = row * inverse
        inner = jnp.where(here, column * inverse, whole - column * scaled)
        gram[...] = jnp.where(there, jnp.where(here, -inverse, scaled), inner)
        return carry

    def loop(first, final, body):
        def step(k, carry):
            body(k)
            return carry

        lax.fori_loop(first, final, step, 0)

    load_d = pltpu.make_async_copy(d_hbm, d, load_sem.at[0])
    load_e = pltpu.make_async_copy(e_hbm, e, load_sem.at[1])
    load_d.start()
    load_e.start()
    barrier = pltpu.get_barrier_semaphore()
    for other in (up, down, sib):
        pl.semaphore_signal(barrier, inc=1, device_id={"samp": other}, device_id_type=MESH)
    xt[me] = xt_ref[...]
    pn_ref[...] = jnp.zeros(pn_ref.shape, F32)
    pl.semaphore_wait(barrier, 3)
    zero = me * 0
    for copy in (x_ring(zero, up, 0, 1), x_ring(zero, down, half, 2), x_across(zero)):
        copy.start()
    load_d.wait()

    def first_picks(q):
        pick(q)
        for copy in own(q):
            copy.start()

    loop(0, 2, first_picks)
    load_e.wait()

    ticks = 2 * last
    total = 4 * ticks

    def tick(t):
        p = lax.div(t, ticks)
        s = lax.div(lax.rem(t, ticks), 2) + 1
        j = lax.rem(t, 2)
        q = 2 * p + j
        chunk_comm(q, s, False)

        @pl.when(jnp.logical_and(t < ticks, j == 0))
        def _():
            x_comm(s, False)

        five, left = lax.div(t, 5), lax.rem(t, 5)

        @pl.when(jnp.logical_and(t < 40, left < 4))
        def _():
            permute(4 * five + left)

        @pl.when(jnp.logical_and(jnp.logical_and(t < 40, left == 4), lax.rem(five, 3) < 2))
        def _():
            first_picks(2 + five - lax.div(five, 3))

        @pl.when(t >= ticks)
        def _():
            chunk_comm(q - 2, s, True)

        @pl.when(t == 29)
        def _():
            gram[...] = jnp.zeros(gram.shape, F32)

            def side(n):
                x_across(n).wait_recv()
                at = 2 * place(n)
                one, two = xt[at], xt[at + 1]
                gram[...] += dot(one, one, (1, 1)) + dot(two, two, (1, 1))

            loop(0, half, side)
            xtm[...] = jnp.zeros(xtm.shape, F32)

        @pl.when(jnp.logical_and(t >= 40, t < 48))
        def _():
            each = covars // 8
            lax.fori_loop((t - 40) * each, (t - 39) * each, sweep, 0)

            def side(n):
                at = 2 * place(n)
                xtm[...] += dot(xt[at], m[2 * n], (1, 0)) + dot(xt[at + 1], m[2 * n + 1], (1, 0))

            loop(2 * (t - 40), 2 * (t - 39), side)

        @pl.when(t == 48)
        def _():
            h[...] = dot(gram[...], xtm[...], (1, 0), HIGHEST)

        @pl.when(t >= 40)
        def _():
            q_old = lax.div(t - 40, 4)
            quarter = lax.rem(t - 40, 4)
            slot = lax.rem(q_old, 3)

            @pl.when(quarter == 0)
            def _():
                @pl.when(q_old >= 3)
                def _():
                    emit(q_old - 3, slot).wait()

                clear(slot)

            loop(4 * quarter, 4 * quarter + 4, lambda n: add(q_old, slot, n))

        @pl.when(t >= 48)
        def _():
            @pl.when(s == 1)
            def _():
                clear(3 + j)

            loop(jnp.maximum(2 * s - 3, 0), 2 * s - 1, lambda n: add(6 + j, 3 + j, n))

        early = jnp.logical_or(t == 49, t == 50)
        regular = jnp.logical_and(t >= 51, lax.rem(t, 4) == 3)

        @pl.when(jnp.logical_or(early, regular))
        def _():
            q_done = jnp.where(early, t - 49, lax.div(t - 43, 4))
            finish_chunk(q_done, lax.rem(q_done, 3))

    loop(0, total, tick)

    def tail(j):
        add(6 + j, 3 + j, end)
        finish_chunk(6 + j, 3 + j)

    loop(0, 2, tail)

    def retire(t):
        s = lax.div(t, 2) + 1
        chunk_comm(6 + lax.rem(t, 2), s, True)

    loop(0, ticks, retire)
    loop(1, last + 1, lambda s: x_comm(s, True))
    for copy in (x_ring(zero, up, 0, 1), x_ring(zero, down, half, 2), x_across(zero)):
        copy.wait_send()

    def retire_own(q):
        for copy in own(q):
            copy.wait_send()

    loop(0, CHUNKS, retire_own)
    loop(3, 8, lambda q: emit(q, jnp.where(q < 6, q - 3, q - 3)).wait())


def local(length, dosage, covariates, expression, block_index, expr_row):
    blocks, width = block_index.shape
    rows, panel = dosage.shape
    covars = covariates.shape[1]
    samples, genes = expression.shape
    wide = blocks * width
    chunk = wide // CHUNKS
    half = length // 2
    scale = math.sqrt(samples - covars - 1)
    vmem = pl.BlockSpec(memory_space=pltpu.VMEM)
    dma = pltpu.SemaphoreType.DMA
    products, panel_norm = pl.pallas_call(
        lambda *refs: scan_kernel(scale, length, *refs),
        out_shape=(
            jax.ShapeDtypeStruct((wide, genes), F32),
            jax.ShapeDtypeStruct((1, genes), F32),
        ),
        in_specs=[pl.BlockSpec(memory_space=pl.ANY)] * 2 + [vmem] * 3,
        out_specs=(pl.BlockSpec(memory_space=pl.ANY), vmem),
        scratch_shapes=[
            pltpu.VMEM((length, wide, rows), BF16),
            pltpu.VMEM((length, covars, rows), BF16),
            pltpu.VMEM((samples, genes), BF16),
            pltpu.VMEM((length, rows, genes), BF16),
            pltpu.VMEM((rows, panel), BF16),
            pltpu.VMEM((5, chunk, genes), F32),
            pltpu.VMEM((5, chunk, covars), F32),
            pltpu.VMEM((5, chunk, min(rows, 128)), F32),
            pltpu.VMEM((rows, genes), F32),
            pltpu.VMEM((rows, chunk), F32),
            pltpu.VMEM((covars, covars), F32),
            pltpu.VMEM((covars, genes), F32),
            pltpu.VMEM((covars, genes), F32),
            dma((CHUNKS, half + 1)),
            dma((CHUNKS, half)),
            dma((CHUNKS, half)),
            dma((CHUNKS, half)),
            dma((half + 1,)),
            dma((half,)),
            dma((half,)),
            dma((half,)),
            dma((2,)),
            dma((CHUNKS,)),
        ],
        compiler_params=pltpu.CompilerParams(
            collective_id=0, has_side_effects=True, vmem_limit_bytes=67000000
        ),
        name="scan",
    )(
        dosage, expression, covariates.T,
        block_index.reshape(CHUNKS, chunk), expr_row.reshape(length, rows),
    )
    return products * lax.rsqrt(panel_norm + epsilon)


def solution(mesh):
    length = mesh.shape["samp"]
    both = ("groups", "samp")
    in_specs = (P(both, None), P(both, None), P("groups", "samp"), P("groups", None), P("groups"))
    return jax.shard_map(
        lambda *args: local(length, *args), mesh=mesh, in_specs=in_specs, out_specs=P("groups", "samp"), check_vma=False
    )
```

```python
import math

import jax
import jax.numpy as jnp
from jax import lax
from jax.experimental import pallas as pl
from jax.experimental.pallas import tpu as pltpu
from jax.sharding import PartitionSpec as P

MESH = pl.DeviceIdType.MESH
HIGHEST = lax.Precision.HIGHEST
F32 = jnp.float32
BF16 = jnp.bfloat16
epsilon = 1e-06
CHUNKS = 4
PARTS = 4


def dot(a, b, contract, precision=None):
    return lax.dot_general(
        a, b, ((contract[:1], contract[1:]), ((), ())), precision=precision, preferred_element_type=F32
    )


def scan_kernel(
    scale, length, per,
    d_hbm, e_hbm, xt_ref, pick_ref, perm_ref,
    out_hbm, pn_ref,
    a, xt, e, m, d, acc, lac, sq, wanted, kacc, gram, xtm, h,
    ring_send, ring_recv, sib_send, sib_recv, x_send, x_recv, xs_send, xs_recv, load_sem, out_sem,
):
    half = length // 2
    last = half // 2
    end = half - 1
    me = lax.axis_index("samp")
    z = lax.div(me, 2)
    core = lax.rem(me, 2)
    up = lax.rem(me + 2, length)
    down = lax.rem(me + length - 2, length)
    sib = me + 1 - 2 * core
    zero = me * 0
    chunk = a.shape[1] // CHUNKS
    rows = a.shape[2]
    pair = 2 * rows
    covars = xt.shape[1]
    panel = d.shape[1] // PARTS
    ring_slots = m.shape[0]

    def place(n):
        s = lax.div(n + 1, 2)
        sign = 2 * lax.rem(n + 1, 2) - 1
        return lax.rem(z + sign * s + half, half)

    def span(q):
        return pl.ds(pl.multiple_of(q * chunk, chunk), chunk)

    def ring(q, n, target, index, arrival):
        ref = a.at[2 * place(n) + core, span(q), :]
        return pltpu.make_async_remote_copy(
            src_ref=ref, dst_ref=ref, send_sem=ring_send.at[q, index], recv_sem=ring_recv.at[q, arrival],
            device_id={"samp": target}, device_id_type=MESH,
        )

    def across(q, n):
        ref = a.at[2 * place(n) + core, span(q), :]
        return pltpu.make_async_remote_copy(
            src_ref=ref, dst_ref=ref, send_sem=sib_send.at[q, n], recv_sem=sib_recv.at[q, n],
            device_id={"samp": sib}, device_id_type=MESH,
        )

    def x_ring(n, target, index, arrival):
        ref = xt.at[2 * place(n) + core]
        return pltpu.make_async_remote_copy(
            src_ref=ref, dst_ref=ref, send_sem=x_send.at[index], recv_sem=x_recv.at[arrival],
            device_id={"samp": target}, device_id_type=MESH,
        )

    def x_across(n):
        ref = xt.at[2 * place(n) + core]
        return pltpu.make_async_remote_copy(
            src_ref=ref, dst_ref=ref, send_sem=xs_send.at[n], recv_sem=xs_recv.at[n],
            device_id={"samp": sib}, device_id_type=MESH,
        )

    def own(q):
        return (ring(q, 0, up, 0, 1), ring(q, 0, down, half, 2), across(q, 0))

    def own_x():
        return (x_ring(zero, up, 0, 1), x_ring(zero, down, half, 2), x_across(zero))

    def comm(s, parity, link, cross, finish):
        def arrive(n, target, forward):
            if not finish:
                link(n, target, n, n).wait_recv()

            @pl.when(forward)
            def _():
                copy = link(n, target, n, jnp.minimum(n + 2, end))
                copy.wait_send() if finish else copy.start()

            copy = cross(n)
            copy.wait_send() if finish else copy.start()

        @pl.when(s < last)
        def _():
            arrive(2 * s - 1, up, jnp.logical_or(s < last - 1, parity == 0))
            arrive(2 * s, down, jnp.logical_or(s < last - 1, parity == 1))

        @pl.when(s == last)
        def _():
            if not finish:
                link(end, up, end, end).wait_recv()
            copy = cross(end)
            copy.wait_send() if finish else copy.start()

    def chunk_comm(q, s, finish=False):
        comm(
            s, lax.rem(q, 2),
            lambda n, target, index, arrival: ring(q, n, target, index, arrival),
            lambda n: across(q, n), finish,
        )

    def x_comm(s, finish=False):
        comm(s, zero, x_ring, x_across, finish)

    def loop(first, final, body):
        def step(k, carry):
            body(k)
            return carry

        lax.fori_loop(first, final, step, 0)

    def load_d(k):
        part = pl.ds(pl.multiple_of(k * panel, panel), panel)
        return pltpu.make_async_copy(d_hbm.at[:, part], d.at[:, part], load_sem.at[k])

    load_e = pltpu.make_async_copy(e_hbm, e, load_sem.at[PARTS])

    def pick(q):
        chosen = pick_ref[pl.ds(lax.div(q, per), 1), span(lax.rem(q, per))]

        def part(k):
            @pl.when(q == 0)
            def _():
                load_d(k).wait()

            start = pl.multiple_of(k * panel, panel)
            spots = lax.broadcasted_iota(jnp.int32, (panel, chunk), 0)
            hot = jnp.where(spots == chosen - start, 1.0, 0.0).astype(BF16)
            piece = dot(d[:, pl.ds(start, panel)], hot, (1, 0))

            @pl.when(k == 0)
            def _():
                kacc[...] = piece

            @pl.when(k > 0)
            def _():
                kacc[...] += piece

        loop(0, PARTS, part)
        a[me, span(q), :] = kacc[...].T.astype(BF16)
        for copy in own(q):
            copy.start()

    def permute(n):
        here = pl.ds(pl.multiple_of(place(n) * pair, pair), pair)
        wanted[...] = jnp.broadcast_to(perm_ref[:, here], (128, pair)).T

        def part(c):
            mine = pl.ds(pl.multiple_of(c * rows, rows), rows)
            spots = lax.broadcasted_iota(jnp.int32, (rows, e.shape[0]), 1)
            hot = jnp.where(spots == wanted[mine, :1], 1.0, 0.0).astype(BF16)
            m[lax.rem(n, ring_slots), mine, :] = dot(hot, e[...], (1, 0)).astype(BF16)

        loop(0, 2, part)
        some = e[pl.ds(pl.multiple_of(n * pair, pair), pair), :].astype(F32)
        pn_ref[...] += jnp.sum(some * some, axis=0, keepdims=True)

    def matched(n):
        both = m[lax.rem(n, ring_slots)]
        return both[:rows], both[rows:]

    def add(q, spots):
        blocks = []
        for n in spots:
            across(q, n).wait_recv()
            at = 2 * place(n)
            mine = matched(n)
            blocks += [(a[at + c, span(q), :], mine[c], xt[at + c]) for c in range(2)]
        acc[q] += sum(dot(block, rest, (1, 0)) for block, rest, _ in blocks)
        lac[q] += sum(dot(block, side, (1, 1)) for block, _, side in blocks)
        total = sum(jnp.square(block.astype(F32)) for block, _, _ in blocks)
        sq[q] += sum(total[:, c : c + sq.shape[2]] for c in range(0, rows, sq.shape[2]))

    def side(n):
        at = 2 * place(n)
        one, two = matched(n)
        xtm[...] += dot(xt[at], one, (1, 0)) + dot(xt[at + 1], two, (1, 0))

    def emit(q):
        return pltpu.make_async_copy(acc.at[q], out_hbm.at[span(q), :], out_sem.at[q])

    def finish_chunk(q):
        loads = lac[q]
        white = dot(loads, gram[...], (1, 0), HIGHEST)
        norm = jnp.sum(sq[q], axis=1, keepdims=True) + jnp.sum(white * loads, axis=1, keepdims=True)
        norm = jnp.maximum(norm, 0.0)
        fitted = dot(loads, h[...], (1, 0), HIGHEST)
        acc[q] = (acc[q] + fitted) * (scale * lax.rsqrt(norm + epsilon))
        emit(q).start()

    def sweep(k):
        whole = gram[...]
        row = gram[pl.ds(k, 1), :]
        here = lax.broadcasted_iota(jnp.int32, whole.shape, 1) == k
        there = lax.broadcasted_iota(jnp.int32, whole.shape, 0) == k
        column = jnp.sum(jnp.where(here, whole, 0.0), axis=1, keepdims=True)
        corner = jnp.sum(jnp.where(here[:1], row, 0.0), axis=1, keepdims=True)
        inverse = 1.0 / corner
        scaled = row * inverse
        inner = jnp.where(here, column * inverse, whole - column * scaled)
        gram[...] = jnp.where(there, jnp.where(here, -inverse, scaled), inner)

    loop(0, PARTS, lambda k: load_d(k).start())
    load_e.start()
    barrier = pltpu.get_barrier_semaphore()
    for other in (up, down, sib):
        pl.semaphore_signal(barrier, inc=1, device_id={"samp": other}, device_id_type=MESH)
    xt[me] = xt_ref[...]
    pl.semaphore_wait(barrier, 3)
    for copy in own_x():
        copy.start()
    loop(0, CHUNKS, pick)
    for ref in (acc, lac, sq, gram, xtm, pn_ref):
        ref[...] = jnp.zeros(ref.shape, F32)
    load_e.wait()
    loop(0, 2, permute)

    ticks = CHUNKS * (last - 1)
    per_tick = covars // 16

    def tick(t):
        s = lax.div(t, CHUNKS) + 1
        j = lax.rem(t, CHUNKS)
        chunk_comm(j, s)

        @pl.when(t < last)
        def _():
            x_comm(t + 1)

        @pl.when(lax.rem(j, 2) == 0)
        def _():
            permute(2 * s + lax.div(j, 2))

        @pl.when(jnp.logical_and(j == 1, s == 1))
        def _():
            x_across(zero).wait_recv()
            side(zero)

        @pl.when(jnp.logical_and(j == 1, s > 1))
        def _():
            @pl.when(s == 2)
            def _():
                loop(1, 3, lambda n: x_across(n).wait_recv())

            loop(2 * s - 3, 2 * s - 1, side)

        @pl.when(jnp.logical_and(lax.rem(j, 2) == 1, s == 1))
        def _():
            loop(j - 1, j + 1, lambda q: add(q, (zero,)))

        @pl.when(jnp.logical_and(lax.rem(j, 2) == 1, s > 1))
        def _():
            loop(j - 1, j + 1, lambda q: add(q, (2 * s - 3, 2 * s - 2)))

        @pl.when(s >= 3)
        def _():
            chunk_comm(j, s - 2, True)

        @pl.when(s == 3)
        def _():
            for copy in own(j):
                copy.wait_send()

        @pl.when(jnp.logical_and(t >= last, t < 2 * last))
        def _():
            x_comm(t - last + 1, True)

        @pl.when(t == last)
        def _():
            for copy in own_x():
                copy.wait_send()

            loop(3, half, lambda n: x_across(n).wait_recv())

            def square(n):
                at = 2 * place(n)
                one, two = xt[at], xt[at + 1]
                gram[...] += dot(one, one, (1, 1)) + dot(two, two, (1, 1))

            loop(0, half, square)

        @pl.when(jnp.logical_and(t > last, t <= last + 16))
        def _():
            loop((t - last - 1) * per_tick, (t - last) * per_tick, sweep)

    loop(0, ticks, tick)

    loop(end - 2, end + 1, side)
    h[...] = dot(gram[...], xtm[...], (1, 0), HIGHEST)
    loop(0, CHUNKS, lambda q: add(q, (zero + end - 2, zero + end - 1)))

    def closing(k):
        first, final = 2 * k, 2 * k + 2
        loop(first, final, lambda q: chunk_comm(q, zero + last))

        def close(q):
            add(q, (zero + end,))
            finish_chunk(q)

        loop(first, final, close)
        loop(0, CHUNKS, lambda q: chunk_comm(q, last - 2 + k, True))

    loop(0, CHUNKS // 2, closing)
    loop(0, CHUNKS, lambda q: chunk_comm(q, zero + last, True))
    loop(0, CHUNKS, lambda q: emit(q).wait())


def local(length, dosage, covariates, expression, block_index, expr_row):
    blocks, width = block_index.shape
    rows, panel = dosage.shape
    covars = covariates.shape[1]
    samples, genes = expression.shape
    wide = blocks * width
    chunk = wide // CHUNKS
    half = length // 2
    scale = math.sqrt(samples - covars - 1)
    vmem = pl.BlockSpec(memory_space=pltpu.VMEM)
    dma = pltpu.SemaphoreType.DMA
    products, panel_norm = pl.pallas_call(
        lambda *refs: scan_kernel(scale, length, CHUNKS // blocks, *refs),
        out_shape=(
            jax.ShapeDtypeStruct((wide, genes), F32),
            jax.ShapeDtypeStruct((1, genes), F32),
        ),
        in_specs=[pl.BlockSpec(memory_space=pl.ANY)] * 2 + [vmem] * 3,
        out_specs=(pl.BlockSpec(memory_space=pl.ANY), vmem),
        scratch_shapes=[
            pltpu.VMEM((length, wide, rows), BF16),
            pltpu.VMEM((length, covars, rows), BF16),
            pltpu.VMEM((samples, genes), BF16),
            pltpu.VMEM((8, 2 * rows, genes), BF16),
            pltpu.VMEM((rows, panel), BF16),
            pltpu.VMEM((CHUNKS, chunk, genes), F32),
            pltpu.VMEM((CHUNKS, chunk, covars), F32),
            pltpu.VMEM((CHUNKS, chunk, min(rows, 128)), F32),
            pltpu.VMEM((2 * rows, 128), jnp.int32),
            pltpu.VMEM((rows, chunk), F32),
            pltpu.VMEM((covars, covars), F32),
            pltpu.VMEM((covars, genes), F32),
            pltpu.VMEM((covars, genes), F32),
            dma((CHUNKS, half + 1)),
            dma((CHUNKS, half)),
            dma((CHUNKS, half)),
            dma((CHUNKS, half)),
            dma((half + 1,)),
            dma((half,)),
            dma((half,)),
            dma((half,)),
            dma((PARTS + 1,)),
            dma((CHUNKS,)),
        ],
        compiler_params=pltpu.CompilerParams(
            collective_id=0, has_side_effects=True, vmem_limit_bytes=67000000
        ),
        name="scan",
    )(
        dosage, expression, covariates.T,
        block_index, expr_row.reshape(1, samples),
    )
    return products * lax.rsqrt(panel_norm + epsilon)


def solution(mesh):
    length = mesh.shape["samp"]
    both = ("groups", "samp")
    in_specs = (P(both, None), P(both, None), P("groups", "samp"), P("groups", None), P("groups"))
    return jax.shard_map(
        lambda *args: local(length, *args), mesh=mesh, in_specs=in_specs, out_specs=P("groups", "samp"), check_vma=False
    )
```

```python
import math

import jax
import jax.numpy as jnp
from jax import lax
from jax.experimental import pallas as pl
from jax.experimental.pallas import tpu as pltpu
from jax.sharding import PartitionSpec as P

MESH = pl.DeviceIdType.MESH
HIGHEST = lax.Precision.HIGHEST
F32 = jnp.float32
BF16 = jnp.bfloat16
epsilon = 1e-06
CHUNKS = 4
PARTS = 4


def dot(a, b, contract, precision=None):
    return lax.dot_general(
        a, b, ((contract[:1], contract[1:]), ((), ())), precision=precision, preferred_element_type=F32
    )


def scan_kernel(
    scale, length, per,
    d_hbm, e_hbm, xt_ref, pick_ref, perm_ref,
    out_ref,
    a, xt, e, m, d, lac, sq, wanted, kacc, gram, xtm, both, pn_ref,
    ring_send, ring_recv, sib_send, sib_recv, x_send, x_recv, xs_send, xs_recv, load_sem,
):
    half = length // 2
    last = half // 2
    end = half - 1
    me = lax.axis_index("samp")
    z = lax.div(me, 2)
    core = lax.rem(me, 2)
    up = lax.rem(me + 2, length)
    down = lax.rem(me + length - 2, length)
    sib = me + 1 - 2 * core
    zero = me * 0
    chunk = a.shape[1] // CHUNKS
    rows = a.shape[2]
    pair = 2 * rows
    covars = xt.shape[1]
    panel = d.shape[1] // PARTS
    ring_slots = m.shape[0]

    def place(n):
        s = lax.div(n + 1, 2)
        sign = 2 * lax.rem(n + 1, 2) - 1
        return lax.rem(z + sign * s + half, half)

    def span(q):
        return pl.ds(pl.multiple_of(q * chunk, chunk), chunk)

    def ring(q, n, target, index, arrival):
        ref = a.at[2 * place(n) + core, span(q), :]
        return pltpu.make_async_remote_copy(
            src_ref=ref, dst_ref=ref, send_sem=ring_send.at[q, index], recv_sem=ring_recv.at[q, arrival],
            device_id={"samp": target}, device_id_type=MESH,
        )

    def across(q, n):
        ref = a.at[2 * place(n) + core, span(q), :]
        return pltpu.make_async_remote_copy(
            src_ref=ref, dst_ref=ref, send_sem=sib_send.at[q, n], recv_sem=sib_recv.at[q, n],
            device_id={"samp": sib}, device_id_type=MESH,
        )

    def x_ring(n, target, index, arrival):
        ref = xt.at[2 * place(n) + core]
        return pltpu.make_async_remote_copy(
            src_ref=ref, dst_ref=ref, send_sem=x_send.at[index], recv_sem=x_recv.at[arrival],
            device_id={"samp": target}, device_id_type=MESH,
        )

    def x_across(n):
        ref = xt.at[2 * place(n) + core]
        return pltpu.make_async_remote_copy(
            src_ref=ref, dst_ref=ref, send_sem=xs_send.at[n], recv_sem=xs_recv.at[n],
            device_id={"samp": sib}, device_id_type=MESH,
        )

    def own(q):
        return (ring(q, 0, up, 0, 1), ring(q, 0, down, half, 2), across(q, 0))

    def own_x():
        return (x_ring(zero, up, 0, 1), x_ring(zero, down, half, 2), x_across(zero))

    def comm(s, parity, link, cross, finish):
        def arrive(n, target, forward):
            if not finish:
                link(n, target, n, n).wait_recv()

            @pl.when(forward)
            def _():
                copy = link(n, target, n, jnp.minimum(n + 2, end))
                copy.wait_send() if finish else copy.start()

            copy = cross(n)
            copy.wait_send() if finish else copy.start()

        @pl.when(s < last)
        def _():
            arrive(2 * s - 1, up, jnp.logical_or(s < last - 1, parity == 0))
            arrive(2 * s, down, jnp.logical_or(s < last - 1, parity == 1))

        @pl.when(s == last)
        def _():
            if not finish:
                link(end, up, end, end).wait_recv()
            copy = cross(end)
            copy.wait_send() if finish else copy.start()

    def chunk_comm(q, s, finish=False):
        comm(
            s, lax.rem(q, 2),
            lambda n, target, index, arrival: ring(q, n, target, index, arrival),
            lambda n: across(q, n), finish,
        )

    def x_comm(s, finish=False):
        comm(s, zero, x_ring, x_across, finish)

    def loop(first, final, body):
        def step(k, carry):
            body(k)
            return carry

        lax.fori_loop(first, final, step, 0)

    def load_d(k):
        part = pl.ds(pl.multiple_of(k * panel, panel), panel)
        return pltpu.make_async_copy(d_hbm.at[:, part], d.at[:, part], load_sem.at[k])

    load_e = pltpu.make_async_copy(e_hbm, e, load_sem.at[PARTS])

    def pick(q):
        chosen = pick_ref[pl.ds(lax.div(q, per), 1), span(lax.rem(q, per))]

        def part(k):
            @pl.when(q == 0)
            def _():
                load_d(k).wait()

            start = pl.multiple_of(k * panel, panel)
            spots = lax.broadcasted_iota(jnp.int32, (panel, chunk), 0)
            hot = jnp.where(spots == chosen - start, 1.0, 0.0).astype(BF16)
            piece = dot(d[:, pl.ds(start, panel)], hot, (1, 0))

            @pl.when(k == 0)
            def _():
                kacc[...] = piece

            @pl.when(k > 0)
            def _():
                kacc[...] += piece

        loop(0, PARTS, part)
        a[me, span(q), :] = kacc[...].T.astype(BF16)
        for copy in own(q):
            copy.start()

    def permute(n):
        here = pl.ds(pl.multiple_of(place(n) * pair, pair), pair)
        wanted[...] = jnp.broadcast_to(perm_ref[:, here], (128, pair)).T

        def part(c):
            mine = pl.ds(pl.multiple_of(c * rows, rows), rows)
            spots = lax.broadcasted_iota(jnp.int32, (rows, e.shape[0]), 1)
            hot = jnp.where(spots == wanted[mine, :1], 1.0, 0.0).astype(BF16)
            m[lax.rem(n, ring_slots), mine, :] = dot(hot, e[...], (1, 0)).astype(BF16)

        loop(0, 2, part)
        some = e[pl.ds(pl.multiple_of(n * pair, pair), pair), :].astype(F32)
        pn_ref[...] += jnp.sum(some * some, axis=0, keepdims=True)

    def matched(n):
        both = m[lax.rem(n, ring_slots)]
        return both[:rows], both[rows:]

    def add(q, spots):
        blocks = []
        for n in spots:
            across(q, n).wait_recv()
            at = 2 * place(n)
            mine = matched(n)
            blocks += [(a[at + c, span(q), :], mine[c], xt[at + c]) for c in range(2)]
        out_ref[span(q), :] += sum(dot(block, rest, (1, 0)) for block, rest, _ in blocks)
        lac[q] += sum(dot(block, side, (1, 1)) for block, _, side in blocks)
        total = sum(jnp.square(block.astype(F32)) for block, _, _ in blocks)
        sq[q] += sum(total[:, c : c + sq.shape[2]] for c in range(0, rows, sq.shape[2]))

    def side(n):
        at = 2 * place(n)
        one, two = matched(n)
        xtm[...] += dot(xt[at], one, (1, 0)) + dot(xt[at + 1], two, (1, 0))

    def finish_chunk(q):
        loads = lac[q]
        change = dot(loads, both[...], (1, 0), HIGHEST)
        genes = xtm.shape[1]
        fitted, white = change[:, :genes], change[:, genes : genes + covars]
        norm = jnp.sum(sq[q], axis=1, keepdims=True) + jnp.sum(white * loads, axis=1, keepdims=True)
        norm = jnp.maximum(norm, 0.0)
        row, column = scale * lax.rsqrt(norm + epsilon), lax.rsqrt(pn_ref[...] + epsilon)
        out_ref[span(q), :] = (out_ref[span(q), :] + fitted) * row * column

    def sweep(k):
        whole = gram[...]
        row = gram[pl.ds(k, 1), :]
        here = lax.broadcasted_iota(jnp.int32, whole.shape, 1) == k
        there = lax.broadcasted_iota(jnp.int32, whole.shape, 0) == k
        column = jnp.sum(jnp.where(here, whole, 0.0), axis=1, keepdims=True)
        corner = jnp.sum(jnp.where(here[:1], row, 0.0), axis=1, keepdims=True)
        inverse = 1.0 / corner
        scaled = row * inverse
        inner = jnp.where(here, column * inverse, whole - column * scaled)
        gram[...] = jnp.where(there, jnp.where(here, -inverse, scaled), inner)

    barrier = pltpu.get_barrier_semaphore()
    for other in (up, down, sib):
        pl.semaphore_signal(barrier, inc=1, device_id={"samp": other}, device_id_type=MESH)
    loop(0, PARTS, lambda k: load_d(k).start())
    xt[me] = xt_ref[...]
    pl.semaphore_wait(barrier, 3)
    for copy in own_x():
        copy.start()
    pick(zero)
    load_e.start()
    loop(1, CHUNKS, pick)
    for ref in (out_ref, lac, sq, gram, xtm, both, pn_ref):
        ref[...] = jnp.zeros(ref.shape, F32)
    load_e.wait()
    loop(0, 2, permute)

    ticks = CHUNKS * (last - 1)
    per_tick = covars // 16

    def tick(t):
        s = lax.div(t, CHUNKS) + 1
        j = lax.rem(t, CHUNKS)
        chunk_comm(j, s)

        @pl.when(t < last)
        def _():
            x_comm(t + 1)

        @pl.when(lax.rem(j, 2) == 0)
        def _():
            permute(2 * s + lax.div(j, 2))

        @pl.when(jnp.logical_and(j == 1, s == 1))
        def _():
            x_across(zero).wait_recv()
            side(zero)

        @pl.when(jnp.logical_and(j == 1, s > 1))
        def _():
            @pl.when(s == 2)
            def _():
                loop(1, 3, lambda n: x_across(n).wait_recv())

            loop(2 * s - 3, 2 * s - 1, side)

        @pl.when(jnp.logical_and(lax.rem(j, 2) == 1, s == 1))
        def _():
            loop(j - 1, j + 1, lambda q: add(q, (zero,)))

        @pl.when(jnp.logical_and(lax.rem(j, 2) == 1, s > 1))
        def _():
            loop(j - 1, j + 1, lambda q: add(q, (2 * s - 3, 2 * s - 2)))

        @pl.when(s >= 3)
        def _():
            chunk_comm(j, s - 2, True)

        @pl.when(s == 3)
        def _():
            for copy in own(j):
                copy.wait_send()

        @pl.when(jnp.logical_and(t >= last, t < 2 * last))
        def _():
            x_comm(t - last + 1, True)

        @pl.when(t == last)
        def _():
            for copy in own_x():
                copy.wait_send()

            loop(3, half, lambda n: x_across(n).wait_recv())

            def square(n):
                at = 2 * place(n)
                one, two = xt[at], xt[at + 1]
                gram[...] += dot(one, one, (1, 1)) + dot(two, two, (1, 1))

            loop(0, half, square)

        @pl.when(jnp.logical_and(t > last, t <= last + 16))
        def _():
            loop((t - last - 1) * per_tick, (t - last) * per_tick, sweep)

    loop(0, ticks, tick)

    loop(end - 2, end + 1, side)
    both[:, : xtm.shape[1]] = dot(gram[...], xtm[...], (1, 0), HIGHEST)
    both[:, xtm.shape[1] : xtm.shape[1] + covars] = gram[...]
    loop(0, CHUNKS, lambda q: add(q, (zero + end - 2, zero + end - 1)))

    def closing(k):
        first, final = 2 * k, 2 * k + 2
        loop(first, final, lambda q: chunk_comm(q, zero + last))

        def close(q):
            add(q, (zero + end,))
            finish_chunk(q)

        loop(first, final, close)
        loop(0, CHUNKS, lambda q: chunk_comm(q, last - 2 + k, True))

    loop(0, CHUNKS // 2, closing)
    loop(0, CHUNKS, lambda q: chunk_comm(q, zero + last, True))


def local(length, dosage, covariates, expression, block_index, expr_row):
    blocks, width = block_index.shape
    rows, panel = dosage.shape
    covars = covariates.shape[1]
    samples, genes = expression.shape
    wide = blocks * width
    chunk = wide // CHUNKS
    half = length // 2
    scale = math.sqrt(samples - covars - 1)
    vmem = pl.BlockSpec(memory_space=pltpu.VMEM)
    dma = pltpu.SemaphoreType.DMA
    return pl.pallas_call(
        lambda *refs: scan_kernel(scale, length, CHUNKS // blocks, *refs),
        out_shape=pltpu.VMEM((wide, genes), F32),
        in_specs=[pl.BlockSpec(memory_space=pl.ANY)] * 2 + [vmem] * 3,
        out_specs=vmem,
        scratch_shapes=[
            pltpu.VMEM((length, wide, rows), BF16),
            pltpu.VMEM((length, covars, rows), BF16),
            pltpu.VMEM((samples, genes), BF16),
            pltpu.VMEM((8, 2 * rows, genes), BF16),
            pltpu.VMEM((rows, panel), BF16),
            pltpu.VMEM((CHUNKS, chunk, covars), F32),
            pltpu.VMEM((CHUNKS, chunk, min(rows, 128)), F32),
            pltpu.VMEM((2 * rows, 128), jnp.int32),
            pltpu.VMEM((rows, chunk), F32),
            pltpu.VMEM((covars, covars), F32),
            pltpu.VMEM((covars, genes), F32),
            pltpu.VMEM((covars, genes + 128), F32),
            pltpu.VMEM((1, genes), F32),
            dma((CHUNKS, half + 1)),
            dma((CHUNKS, half)),
            dma((CHUNKS, half)),
            dma((CHUNKS, half)),
            dma((half + 1,)),
            dma((half,)),
            dma((half,)),
            dma((half,)),
            dma((PARTS + 1,)),
        ],
        compiler_params=pltpu.CompilerParams(
            collective_id=0, has_side_effects=True, vmem_limit_bytes=62000000
        ),
        name="scan",
    )(
        dosage, expression, covariates.T,
        block_index, expr_row.reshape(1, samples),
    )


def solution(mesh):
    length = mesh.shape["samp"]
    both = ("groups", "samp")
    in_specs = (P(both, None), P(both, None), P("groups", "samp"), P("groups", None), P("groups"))
    return jax.shard_map(
        lambda *args: local(length, *args), mesh=mesh, in_specs=in_specs, out_specs=P("groups", "samp"), check_vma=False
    )
```

```python
import math

import jax
import jax.numpy as jnp
from jax import lax
from jax.experimental import pallas as pl
from jax.experimental.pallas import tpu as pltpu
from jax.sharding import PartitionSpec as P

MESH = pl.DeviceIdType.MESH
HIGHEST = lax.Precision.HIGHEST
F32 = jnp.float32
BF16 = jnp.bfloat16
epsilon = 1e-06
CHUNKS = 4
PARTS = 4


def dot(a, b, contract, precision=None):
    return lax.dot_general(
        a, b, ((contract[:1], contract[1:]), ((), ())), precision=precision, preferred_element_type=F32
    )


def scan_kernel(
    scale, length, per,
    d_hbm, e_hbm, xt_ref, pick_ref, perm_ref,
    out_ref,
    a, xt, e, m, d, lac, sq, wanted, kacc, gram, xtm, both, terms, pn_ref,
    ring_send, ring_recv, sib_send, sib_recv, x_send, x_recv, xs_send, xs_recv, load_sem,
):
    half = length // 2
    last = half // 2
    end = half - 1
    me = lax.axis_index("samp")
    z = lax.div(me, 2)
    core = lax.rem(me, 2)
    up = lax.rem(me + 2, length)
    down = lax.rem(me + length - 2, length)
    sib = me + 1 - 2 * core
    zero = me * 0
    chunk = a.shape[1] // CHUNKS
    rows = a.shape[2]
    pair = 2 * rows
    covars = xt.shape[1]
    panel = d.shape[1] // PARTS
    ring_slots = m.shape[0]

    def place(n):
        s = lax.div(n + 1, 2)
        sign = 2 * lax.rem(n + 1, 2) - 1
        return lax.rem(z + sign * s + half, half)

    def span(q):
        return pl.ds(pl.multiple_of(q * chunk, chunk), chunk)

    def ring(q, n, target, index, arrival):
        ref = a.at[2 * place(n) + core, span(q), :]
        return pltpu.make_async_remote_copy(
            src_ref=ref, dst_ref=ref, send_sem=ring_send.at[q, index], recv_sem=ring_recv.at[q, arrival],
            device_id={"samp": target}, device_id_type=MESH,
        )

    def across(q, n):
        ref = a.at[2 * place(n) + core, span(q), :]
        return pltpu.make_async_remote_copy(
            src_ref=ref, dst_ref=ref, send_sem=sib_send.at[q, n], recv_sem=sib_recv.at[q, n],
            device_id={"samp": sib}, device_id_type=MESH,
        )

    small = chunk // 2

    def half_span(q, part):
        return pl.ds(pl.multiple_of(q * chunk + part * small, small), small)

    def last_ring(q, n, target, part):
        ref = a.at[2 * place(n) + core, half_span(q, part), :]
        return pltpu.make_async_remote_copy(
            src_ref=ref, dst_ref=ref, send_sem=ring_send.at[q, n if part == 0 else half + 1],
            recv_sem=ring_recv.at[q, end + part], device_id={"samp": target}, device_id_type=MESH,
        )

    def last_across(q, part):
        ref = a.at[2 * place(zero + end) + core, half_span(q, part), :]
        return pltpu.make_async_remote_copy(
            src_ref=ref, dst_ref=ref, send_sem=sib_send.at[q, end + part], recv_sem=sib_recv.at[q, end + part],
            device_id={"samp": sib}, device_id_type=MESH,
        )

    def x_ring(n, target, index, arrival):
        ref = xt.at[2 * place(n) + core]
        return pltpu.make_async_remote_copy(
            src_ref=ref, dst_ref=ref, send_sem=x_send.at[index], recv_sem=x_recv.at[arrival],
            device_id={"samp": target}, device_id_type=MESH,
        )

    def x_across(n):
        ref = xt.at[2 * place(n) + core]
        return pltpu.make_async_remote_copy(
            src_ref=ref, dst_ref=ref, send_sem=xs_send.at[n], recv_sem=xs_recv.at[n],
            device_id={"samp": sib}, device_id_type=MESH,
        )

    def own(q):
        return (ring(q, 0, up, 0, 1), ring(q, 0, down, half, 2), across(q, 0))

    def own_x():
        return (x_ring(zero, up, 0, 1), x_ring(zero, down, half, 2), x_across(zero))

    def comm(s, parity, link, cross, finish, q=None):
        def go(copy):
            copy.wait_send() if finish else copy.start()

        def arrive(n, target, mine):
            if not finish:
                link(n, target, n, n).wait_recv()
            whole = s < last - 1
            tip = jnp.logical_and(s == last - 1, mine)

            @pl.when(whole if q is not None else jnp.logical_or(whole, tip))
            def _():
                go(link(n, target, n, jnp.minimum(n + 2, end)))

            if q is not None:
                @pl.when(tip)
                def _():
                    for part in range(2):
                        go(last_ring(q, n, target, part))

            go(cross(n))

        @pl.when(s < last)
        def _():
            arrive(2 * s - 1, up, parity == 0)
            arrive(2 * s, down, parity == 1)

        if q is None:
            @pl.when(s == last)
            def _():
                if not finish:
                    link(end, up, end, end).wait_recv()
                go(cross(end))

    def chunk_comm(q, s, finish=False):
        comm(
            s, lax.rem(q, 2),
            lambda n, target, index, arrival: ring(q, n, target, index, arrival),
            lambda n: across(q, n), finish, q,
        )

    def x_comm(s, finish=False):
        comm(s, zero, x_ring, x_across, finish)

    def loop(first, final, body):
        def step(k, carry):
            body(k)
            return carry

        lax.fori_loop(first, final, step, 0)

    def load_d(k):
        part = pl.ds(pl.multiple_of(k * panel, panel), panel)
        return pltpu.make_async_copy(d_hbm.at[:, part], d.at[:, part], load_sem.at[k])

    load_e = pltpu.make_async_copy(e_hbm, e, load_sem.at[PARTS])

    def pick(q):
        chosen = pick_ref[pl.ds(lax.div(q, per), 1), span(lax.rem(q, per))]

        def part(k):
            @pl.when(q == 0)
            def _():
                load_d(k).wait()

            start = pl.multiple_of(k * panel, panel)
            spots = lax.broadcasted_iota(jnp.int32, (panel, chunk), 0)
            hot = jnp.where(spots == chosen - start, 1.0, 0.0).astype(BF16)
            piece = dot(d[:, pl.ds(start, panel)], hot, (1, 0))

            @pl.when(k == 0)
            def _():
                kacc[...] = piece

            @pl.when(k > 0)
            def _():
                kacc[...] += piece

        loop(0, PARTS, part)
        a[me, span(q), :] = kacc[...].T.astype(BF16)
        for copy in own(q):
            copy.start()

    def permute(n):
        here = pl.ds(pl.multiple_of(place(n) * pair, pair), pair)
        wanted[...] = jnp.broadcast_to(perm_ref[:, here], (128, pair)).T

        def part(c):
            mine = pl.ds(pl.multiple_of(c * rows, rows), rows)
            spots = lax.broadcasted_iota(jnp.int32, (rows, e.shape[0]), 1)
            hot = jnp.where(spots == wanted[mine, :1], 1.0, 0.0).astype(BF16)
            m[lax.rem(n, ring_slots), mine, :] = dot(hot, e[...], (1, 0)).astype(BF16)

        loop(0, 2, part)

    def measure(n):
        some = e[pl.ds(pl.multiple_of(n * pair, pair), pair), :].astype(F32)
        pn_ref[...] += jnp.sum(some * some, axis=0, keepdims=True)

    def matched(n):
        both = m[lax.rem(n, ring_slots)]
        return both[:rows], both[rows:]

    def collect(here, spots):
        blocks = []
        for n in spots:
            at = 2 * place(n)
            mine = matched(n)
            blocks += [(a[at + c, here, :], mine[c], xt[at + c]) for c in range(2)]
        out_ref[here, :] += sum(dot(block, rest, (1, 0)) for block, rest, _ in blocks)
        lac[here, :covars] += sum(dot(block, side, (1, 1)) for block, _, side in blocks)
        total = sum(jnp.square(block.astype(F32)) for block, _, _ in blocks)
        sq[here, :] += sum(total[:, c : c + sq.shape[1]] for c in range(0, rows, sq.shape[1]))

    def add(q, spots):
        for n in spots:
            across(q, n).wait_recv()
        collect(span(q), spots)

    def side(n):
        at = 2 * place(n)
        one, two = matched(n)
        xtm[...] += dot(xt[at], one, (1, 0)) + dot(xt[at + 1], two, (1, 0))

    def split(x):
        high = x.astype(BF16)
        rest = x - high.astype(F32)
        middle = rest.astype(BF16)
        return high, middle, (rest - middle.astype(F32)).astype(BF16)

    def finish(here):
        loads = lac[here, :]
        high, middle, low = split(loads)
        one, two = jnp.concatenate([high, middle], axis=1), jnp.concatenate([high, low], axis=1)
        change = dot(one, terms[0], (1, 0)) + (dot(one, terms[1], (1, 0)) + dot(two, terms[2], (1, 0)))
        genes = xtm.shape[1]
        fitted, white = change[:, :genes], change[:, genes:]
        norm = jnp.sum(sq[here, :], axis=1, keepdims=True) + jnp.sum(white * loads, axis=1, keepdims=True)
        norm = jnp.maximum(norm, 0.0)
        row, column = scale * lax.rsqrt(norm + epsilon), lax.rsqrt(pn_ref[...] + epsilon)
        out_ref[here, :] = (out_ref[here, :] + fitted) * row * column

    def sweep(k):
        whole = gram[...]
        row = gram[pl.ds(k, 1), :]
        here = lax.broadcasted_iota(jnp.int32, whole.shape, 1) == k
        there = lax.broadcasted_iota(jnp.int32, whole.shape, 0) == k
        column = jnp.sum(jnp.where(here, whole, 0.0), axis=1, keepdims=True)
        corner = jnp.sum(jnp.where(here[:1], row, 0.0), axis=1, keepdims=True)
        inverse = 1.0 / corner
        scaled = row * inverse
        inner = jnp.where(here, column * inverse, whole - column * scaled)
        gram[...] = jnp.where(there, jnp.where(here, -inverse, scaled), inner)

    barrier = pltpu.get_barrier_semaphore()
    for other in (up, down, sib):
        pl.semaphore_signal(barrier, inc=1, device_id={"samp": other}, device_id_type=MESH)
    loop(0, PARTS, lambda k: load_d(k).start())
    xt[me] = xt_ref[...]
    pl.semaphore_wait(barrier, 3)
    for copy in own_x():
        copy.start()
    pick(zero)
    load_e.start()
    loop(1, CHUNKS, pick)
    for ref in (out_ref, lac, sq, gram, xtm, both, pn_ref):
        ref[...] = jnp.zeros(ref.shape, F32)
    load_e.wait()
    permute(zero)

    ticks = CHUNKS * (last - 1)
    per_tick = covars // 8

    def tick(t):
        s = lax.div(t, CHUNKS) + 1
        j = lax.rem(t, CHUNKS)
        chunk_comm(j, s)

        @pl.when(t < last)
        def _():
            x_comm(t + 1)

        @pl.when(lax.rem(j, 2) == 0)
        def _():
            permute(2 * s + lax.div(j, 2))

        @pl.when(t == 1)
        def _():
            permute(zero + 1)

        @pl.when(jnp.logical_and(j == 1, s == 1))
        def _():
            x_across(zero).wait_recv()
            side(zero)

        @pl.when(jnp.logical_and(j == 1, s > 1))
        def _():
            @pl.when(s == 2)
            def _():
                loop(1, 3, lambda n: x_across(n).wait_recv())

            loop(2 * s - 3, 2 * s - 1, side)

        @pl.when(jnp.logical_and(lax.rem(j, 2) == 1, s == 1))
        def _():
            loop(j - 1, j + 1, lambda q: add(q, (zero,)))

        @pl.when(jnp.logical_and(lax.rem(j, 2) == 1, s > 1))
        def _():
            loop(j - 1, j + 1, lambda q: add(q, (2 * s - 3, 2 * s - 2)))

        @pl.when(s >= 3)
        def _():
            chunk_comm(j, s - 2, True)

        @pl.when(s == 3)
        def _():
            for copy in own(j):
                copy.wait_send()

        @pl.when(jnp.logical_and(t >= last, t < 2 * last))
        def _():
            x_comm(t - last + 1, True)

        @pl.when(t == last)
        def _():
            for copy in own_x():
                copy.wait_send()

            loop(3, half, lambda n: x_across(n).wait_recv())

        @pl.when(t == last + 1)
        def _():
            def square(n):
                at = 2 * place(n)
                one, two = xt[at], xt[at + 1]
                gram[...] += dot(one, one, (1, 1)) + dot(two, two, (1, 1))

            loop(0, half, square)

        odd = lax.rem(j, 2) == 1

        @pl.when(odd)
        def _():
            measure(2 * s + lax.div(j, 2))

        @pl.when(t == 3)
        def _():
            loop(0, 2, measure)

        @pl.when(jnp.logical_and(odd, jnp.logical_and(t > last + 2, t < last + 18)))
        def _():
            turn = lax.div(t - last - 3, 2)
            loop(turn * per_tick, (turn + 1) * per_tick, sweep)

    loop(0, ticks, tick)

    loop(end - 2, end + 1, side)
    both[:covars, : xtm.shape[1]] = dot(gram[...], xtm[...], (1, 0), HIGHEST)
    both[:covars, xtm.shape[1] : xtm.shape[1] + covars] = gram[...]
    high, middle, low = split(both[...])
    terms[0] = jnp.concatenate([high, high], axis=0)
    terms[1] = jnp.concatenate([middle, middle], axis=0)
    terms[2] = jnp.concatenate([low, high], axis=0)
    loop(0, CHUNKS, lambda q: add(q, (zero + end - 2, zero + end - 1)))

    for k in range(CHUNKS // 2):
        for part in range(2):
            def land(q):
                copy = last_ring(q, zero + end, up, part)
                copy.wait_recv()
                last_across(q, part).start()

            def close(q):
                last_across(q, part).wait_recv()
                collect(half_span(q, part), (zero + end,))
                finish(half_span(q, part))

            loop(2 * k, 2 * k + 2, land)
            loop(2 * k, 2 * k + 2, close)
        loop(0, CHUNKS, lambda q: chunk_comm(q, zero + last - 2 + k, True))

    def retire(q):
        for part in range(2):
            last_across(q, part).wait_send()

    loop(0, CHUNKS, retire)


def local(length, dosage, covariates, expression, block_index, expr_row):
    blocks, width = block_index.shape
    rows, panel = dosage.shape
    covars = covariates.shape[1]
    samples, genes = expression.shape
    wide = blocks * width
    chunk = wide // CHUNKS
    half = length // 2
    scale = math.sqrt(samples - covars - 1)
    vmem = pl.BlockSpec(memory_space=pltpu.VMEM)
    dma = pltpu.SemaphoreType.DMA
    return pl.pallas_call(
        lambda *refs: scan_kernel(scale, length, CHUNKS // blocks, *refs),
        out_shape=pltpu.VMEM((wide, genes), F32),
        in_specs=[pl.BlockSpec(memory_space=pl.ANY)] * 2 + [vmem] * 3,
        out_specs=vmem,
        scratch_shapes=[
            pltpu.VMEM((length, wide, rows), BF16),
            pltpu.VMEM((length, covars, rows), BF16),
            pltpu.VMEM((samples, genes), BF16),
            pltpu.VMEM((8, 2 * rows, genes), BF16),
            pltpu.VMEM((rows, panel), BF16),
            pltpu.VMEM((wide, 128), F32),
            pltpu.VMEM((wide, 128), F32),
            pltpu.VMEM((2 * rows, 128), jnp.int32),
            pltpu.VMEM((rows, chunk), F32),
            pltpu.VMEM((covars, covars), F32),
            pltpu.VMEM((covars, genes), F32),
            pltpu.VMEM((128, genes + 128), F32),
            pltpu.VMEM((3, 256, genes + 128), BF16),
            pltpu.VMEM((1, genes), F32),
            dma((CHUNKS, half + 2)),
            dma((CHUNKS, half + 1)),
            dma((CHUNKS, half + 1)),
            dma((CHUNKS, half + 1)),
            dma((half + 1,)),
            dma((half,)),
            dma((half,)),
            dma((half,)),
            dma((PARTS + 1,)),
        ],
        compiler_params=pltpu.CompilerParams(
            collective_id=0, has_side_effects=True, vmem_limit_bytes=62000000
        ),
        name="scan",
    )(
        dosage, expression, covariates.T,
        block_index, expr_row.reshape(1, samples),
    )


def solution(mesh):
    length = mesh.shape["samp"]
    both = ("groups", "samp")
    in_specs = (P(both, None), P(both, None), P("groups", "samp"), P("groups", None), P("groups"))
    return jax.shard_map(
        lambda *args: local(length, *args), mesh=mesh, in_specs=in_specs, out_specs=P("groups", "samp"), check_vma=False
    )
```
